256 devices in a mesh: parts: 4 (over x, y), owner: 64 (over z, core).
Axes of the slice: x: 2, y: 2, z: 32, core: 2. Of those that a mesh axis runs over, the one named last changes fastest.
The devices are a block of a 4x8x32 slice.
Arguments:
- embeddings: bfloat16 [1048576, 512], P(('parts', 'owner')), parts along dimension 0, may hold values from -6 to 6
- cluster: int32 [1048576], P(('parts', 'owner')), parts along dimension 0, may hold values from 0 to 7
- lengths: int32 [256, 64], P(('parts', 'owner')), parts along dimension 0, may hold values from 1 to 64, 3584 in all within a row
Outputs:
- best: float32 [1048576], P(('parts', 'owner')), parts along dimension 0
The draws below stay inside these ranges and needn't reach their ends.
There are 4 independent parts, one for each index of `parts`. The reference program is written for one: setup_inputs(seed, part) draws one part's arguments, and reference() takes and returns one part's arrays. A program takes and returns all parts, laid end to end along the dimension named above; each array names one. Nothing has to cross between parts.
Inputs may be any that keep to these rules, and one draw needn't show every extreme that they name: Each row of lengths sums to 3584 and reaches 64 in some column.
All inputs are finite; a program needn't handle non-finite values.
Results may differ from the reference program's by a relative error of at most 0.00049.
Values may be sent and summed in bfloat16 or wider, within the bound.
A program may use at most 64 MiB of HBM per device.

```python
import math
import jax
import jax.numpy as jnp
import numpy as np
from jax import lax

E = 512
CAP = 64
C_DEV = 8
ROWS = 262144
N_OWNER = 64


def touch_ends(drawn, rng, smallest, high):
    longest = drawn.shape.index(max(drawn.shape))
    spots = []
    for shift in (0, 1):
        where = [jax.random.randint(jax.random.fold_in(rng, axis), (), 0, length) for axis, length in enumerate(drawn.shape)]
        where[longest] = (where[longest] + shift) % drawn.shape[longest]
        spots.append(tuple(where))
    return drawn.at[spots[0]].set(smallest).at[spots[1]].set(high)


def steps_of(own_key, shape, shards, low, top_value):
    def one(axis_at, parts):
        heights = jax.random.uniform(jax.random.fold_in(jax.random.fold_in(own_key, 6), axis_at), (parts,), jnp.float32, low / len(shards), top_value / len(shards))
        return jnp.repeat(jnp.exp(heights), shape[axis_at] // parts).reshape((-1,) + (1,) * (len(shape) - axis_at - 1))

    level = one(*shards[0])
    for cut in shards[1:]:
        level = level * one(*cut)
    return level


def rank_table(count, skew):
    loads = [(1 << 20) // math.isqrt(standing ** skew) + 1 for standing in range(1, count + 1)]
    spread = 1 + sum(loads) // (1 << 30)
    return np.cumsum(np.array([max(1, weight // spread) for weight in loads]))


def skewed_ids(stream_key, shape, amount, lean):
    grid = rank_table(amount, lean)
    ticket = jax.random.randint(jax.random.fold_in(stream_key, 1), shape, 0, int(grid[amount - 1]))
    rank = jnp.searchsorted(jnp.asarray(grid, jnp.int32), ticket, side="right")
    return jax.random.permutation(jax.random.fold_in(stream_key, 2), amount)[rank].astype(jnp.int32)


def profile(count, total, reach, slope):
    portions = [(1 << 20) // math.isqrt(standing ** slope) + 1 for standing in range(2, count + 1)]
    rest, given = total - reach - (count - 1), [1] * (count - 1)
    while rest > 0:
        candidates = [i for i in range(count - 1) if given[i] < reach]
        mass, remaining = sum([portions[i] for i in candidates]), rest
        for i in candidates:
            extra = min(reach - given[i], max(1, remaining * portions[i] // mass), rest)
            given[i] = given[i] + extra
            rest = rest - extra
    return np.array([reach] + given)


def uneven_parts(stream_key, number_of, total, most, skew):
    if number_of == 2:
        one = jax.random.randint(stream_key, (), max(1, total - most), min(most, total - 1) + 1)
        return jnp.stack([one, total - one])
    sizes = jnp.asarray(profile(number_of, total, most, skew), jnp.int32)
    couples = (number_of - 1) // 2
    source_of, sink = sizes[1:1 + 2 * couples:2], sizes[2:2 + 2 * couples:2]
    room = jnp.minimum(source_of - 1, most - sink)
    shifted = jax.random.randint(jax.random.fold_in(stream_key, 1), (couples,), 0, 1 << 20) % (room + 1)
    sizes = sizes.at[1:1 + 2 * couples:2].set(source_of - shifted).at[2:2 + 2 * couples:2].set(sink + shifted)
    return sizes[jax.random.permutation(jax.random.fold_in(stream_key, 2), number_of)]


def centred(rng, dims, scale, bound, shards=(), kind=jnp.bfloat16):
    result = jax.random.normal(rng, dims, jnp.float32) * scale
    if len(shards) > 0:
        result = steps_of(rng, dims, shards, -0.22, 0.18) * result
    return jnp.clip(result, min=-bound, max=bound).astype(kind)


def setup_inputs(seed: int = 0, part: int = 0) -> dict:
    keys = jax.random.split(jax.random.key(seed), 4)
    own_keys = jax.random.split(jax.random.fold_in(keys[3], part), 4)
    embeddings = centred(own_keys[0], (ROWS, E), 1.0, 6.0, ((0, 64),))
    cluster = touch_ends(skewed_ids(own_keys[1], (ROWS,), C_DEV, 2), jax.random.fold_in(own_keys[1], 3), 0, C_DEV - 1).astype(jnp.int32)
    lengths = jax.vmap(lambda own: uneven_parts(own, N_OWNER, N_OWNER * CAP - N_OWNER * CAP // 8, CAP, 2))(jax.random.split(own_keys[2], N_OWNER)).reshape((N_OWNER, N_OWNER)).astype(jnp.int32)
    return {"embeddings": embeddings, "cluster": cluster, "lengths": lengths}


def normalize(embeddings):
    values = embeddings.astype(jnp.float32)
    factor = lax.rsqrt(lax.optimization_barrier(jnp.mean(values * values, axis=-1, keepdims=True)) + 1e-06) / math.sqrt(E)
    return (values * factor).astype(jnp.bfloat16)

def owner_best(pair):
    units, labels = pair
    similar = jnp.dot(units, units.T, preferred_element_type=jnp.float32)
    count = units.shape[0]
    index = jnp.arange(count, dtype=jnp.int32)
    same_group = (labels[:, None] == labels[None, :]) & (labels[:, None] >= 0) & (index[:, None] != index[None, :])
    return lax.optimization_barrier(jnp.max(jnp.where(same_group, similar, jnp.float32(-1.0)), axis=1))

def reference(embeddings, cluster, lengths):
    owners = N_OWNER
    units = normalize(embeddings)
    total = owners * owners * CAP
    slots = jnp.arange(total, dtype=jnp.int32)
    limits = jnp.repeat(lengths.reshape(-1), CAP, total_repeat_length=total)
    live = slots % CAP < limits
    labels = jnp.where(live, cluster, -1).astype(jnp.int32)
    grouped = units.reshape(owners, owners, CAP, E).transpose(1, 0, 2, 3).reshape(owners, owners * CAP, E)
    grouped_labels = labels.reshape(owners, owners, CAP).transpose(1, 0, 2).reshape(owners, owners * CAP)
    results = lax.map(owner_best, (grouped, grouped_labels))
    return results.reshape(owners, owners, CAP).transpose(1, 0, 2).reshape(total)
```

```python
import math

import jax
import jax.numpy as jnp
from jax import lax
from jax.experimental import pallas as pl
from jax.experimental.pallas import tpu as pltpu
from jax.sharding import PartitionSpec as P

AHEAD = 16
GROUP = 4
OWNER = "owner"


def exchange_kernel(
    owners, emb_hbm, lab_ref, out_ref,
    emb_v, land, units, lab_land, labrow, labcol, rowacc, colbest, res_out, res_land,
    load_sem, self_sem, send_sem, recv_sem, lab_send, lab_recv, res_send, res_recv,
):
    chips = owners // 2
    far = chips // 2
    cap = land.shape[1]
    width = land.shape[2]
    tile = 4 * cap
    half_tile = 2 * cap
    me = lax.axis_index(OWNER)
    core = lax.rem(me, 2)
    chip = me // 2

    load = pltpu.make_async_copy(emb_hbm, emb_v, load_sem)
    load.start()

    barrier = pltpu.get_barrier_semaphore()

    def greet(i, _):
        pl.semaphore_signal(barrier, inc=1, device_id={OWNER: lax.rem(me + i, owners)})
        return 0

    lax.fori_loop(1, owners, greet, 0)

    labcol[...] = jnp.full_like(labcol, -2)
    rowacc[...] = jnp.full_like(rowacc, -1.0)

    pl.semaphore_wait(barrier, owners - 1)
    load.wait()

    def block_copy(dest, slot, land_slot):
        return pltpu.make_async_remote_copy(
            src_ref=emb_v.at[pl.ds(pl.multiple_of(dest * cap, cap), cap)],
            dst_ref=land.at[land_slot],
            send_sem=send_sem.at[slot],
            recv_sem=recv_sem.at[land_slot],
            device_id={OWNER: dest},
        )

    def label_copy(dest, slot, land_slot):
        return pltpu.make_async_remote_copy(
            src_ref=lab_ref.at[dest],
            dst_ref=lab_land.at[land_slot],
            send_sem=lab_send.at[slot],
            recv_sem=lab_recv.at[land_slot],
            device_id={OWNER: dest},
        )

    def start(dest, slot, land_slot):
        label_copy(dest, slot, land_slot).start()
        block_copy(dest, slot, land_slot).start()

    def send_phase(t):
        k = far - t
        right = lax.rem(chip + k, chips)
        left = lax.rem(chip + chips - k, chips)
        for c in range(2):
            start(right * 2 + c, t * 4 + c, t * 4 + core)
            start(left * 2 + c, t * 4 + 2 + c, t * 4 + 2 + core)

    keep = pltpu.make_async_copy(
        emb_v.at[pl.ds(pl.multiple_of(me * cap, cap), cap)], land.at[core], self_sem.at[0])
    keep_lab = pltpu.make_async_copy(lab_ref.at[me], lab_land.at[core], self_sem.at[1])
    keep.start()
    keep_lab.start()
    partner = chip * 2 + 1 - core
    start(partner, 0, core)
    opposite = lax.rem(chip + far, chips)
    for c in range(2):
        start(opposite * 2 + c, 2 + c, 2 + core)

    def issue(t, _):
        send_phase(t)
        return 0

    lax.fori_loop(1, min(AHEAD, far), issue, 0)

    def arrived(slot):
        label_copy(me, slot, slot).wait_recv()
        block_copy(me, slot, slot).wait_recv()

    def best_of(t):
        for h in range(2):
            row = jnp.maximum(lab_land[4 * t + 2 * h], lab_land[4 * t + 2 * h + 1])
            labrow[2 * t + h] = row
            spread = jnp.broadcast_to(row, (half_tile, half_tile))
            column = jnp.transpose(spread)
            labcol[pl.ds(pl.multiple_of(t * tile + h * half_tile, half_tile), half_tile), :] = jnp.where(
                column < 0, -2, column)
        values = land[pl.ds(4 * t, 4)].reshape(tile, width).astype(jnp.float32)
        factor = lax.rsqrt(jnp.mean(values * values, axis=-1, keepdims=True) + 1e-06) / math.sqrt(width)
        new = (values * factor).astype(jnp.bfloat16)
        units[pl.ds(pl.multiple_of(t * tile, tile), tile), :] = new

        def group(g, running, diagonal):
            span = GROUP * tile
            rows = pl.ds(pl.multiple_of(g * span, span), span)
            old = units[rows, :]
            fresh = units[pl.ds(pl.multiple_of(t * tile, tile), tile), :]
            sim = lax.dot_general(
                old, fresh, (((1,), (1,)), ((), ())), preferred_element_type=jnp.float32)
            col = labcol[rows, :]
            acc = rowacc[rows, :]
            out = []
            for h in range(2):
                part = sim[:, h * half_tile:(h + 1) * half_tile]
                same = col == labrow[2 * t + h]
                if diagonal:
                    i = g * span + lax.broadcasted_iota(jnp.int32, part.shape, 0)
                    j = t * tile + h * half_tile + lax.broadcasted_iota(jnp.int32, part.shape, 1)
                    same = same & (i != j)
                part = jnp.where(same, part, -1.0)
                acc = jnp.maximum(acc, part)
                out.append(jnp.maximum(running[h], jnp.max(part, axis=0, keepdims=True)))
            rowacc[rows, :] = acc
            return tuple(out)

        floor = jnp.full((1, half_tile), -1.0, jnp.float32)
        running = lax.fori_loop(0, t // GROUP, lambda g, r: group(g, r, False), (floor, floor))
        running = group(t // GROUP, running, True)
        for h in range(2):
            colbest[2 * t + h] = running[h]

    keep.wait()
    keep_lab.wait()
    arrived(1 - core)
    arrived(2)
    arrived(3)
    best_of(0)

    def step(t, _):
        @pl.when(t + AHEAD - 1 < far)
        def _():
            send_phase(t + AHEAD - 1)
        for s in range(4):
            arrived(4 * t + s)
        best_of(t)
        return 0

    lax.fori_loop(1, far, step, 0)

    def finish(i, _):
        block = rowacc[pl.ds(pl.multiple_of(i * half_tile, half_tile), half_tile), :]
        late = jnp.max(jnp.transpose(block), axis=0, keepdims=True)
        res_out[i] = jnp.maximum(colbest[i], late)
        return 0

    lax.fori_loop(0, chips, finish, 0)

    def result_copy(row, dest, slot):
        return pltpu.make_async_remote_copy(
            src_ref=res_out.at[row],
            dst_ref=res_land.at[me],
            send_sem=res_send.at[slot],
            recv_sem=res_recv.at[me],
            device_id={OWNER: dest},
        )

    for c in range(2):
        result_copy(1, opposite * 2 + c, 2 + c).start()

    def give(t, _):
        k = far - t
        right = lax.rem(chip + k, chips)
        left = lax.rem(chip + chips - k, chips)
        for c in range(2):
            result_copy(2 * t, left * 2 + c, t * 4 + c).start()
            result_copy(2 * t + 1, right * 2 + c, t * 4 + 2 + c).start()
        return 0

    lax.fori_loop(1, far, give, 0)
    result_copy(0, partner, 0).start()
    res_land[me] = res_out[0]

    def back(i, _):
        s = lax.rem(me + i, owners)
        pltpu.make_async_remote_copy(
            src_ref=res_out.at[0], dst_ref=res_land.at[s], send_sem=res_send.at[0],
            recv_sem=res_recv.at[s], device_id={OWNER: s},
        ).wait_recv()
        return 0

    lax.fori_loop(1, owners, back, 0)

    lane = lax.broadcasted_iota(jnp.int32, (1, half_tile), 1)
    for k in range(chips):
        low, high = res_land[2 * k], res_land[2 * k + 1]
        low = jnp.where(core == 0, low, pltpu.roll(low, cap, 1))
        high = jnp.where(core == 0, pltpu.roll(high, cap, 1), high)
        out_ref[k:k + 1, :] = jnp.where(lane < cap, low, high)

    def sent(slot, _):
        block_copy(me, slot, slot).wait_send()
        label_copy(me, slot, slot).wait_send()
        result_copy(0, me, slot).wait_send()
        return 0

    sent(0, 0)
    lax.fori_loop(2, owners, sent, 0)


def on_device(embeddings, cluster, lengths):
    owners = lax.axis_size(OWNER)
    rows_here, width = embeddings.shape
    cap = rows_here // owners
    chips = owners // 2
    core = lax.rem(lax.axis_index(OWNER), 2)
    slot = lax.broadcasted_iota(jnp.int32, (owners, cap), 1)
    labels = jnp.where(slot < lengths.reshape(owners, 1), cluster.reshape(owners, cap), -1)
    lane = lax.broadcasted_iota(jnp.int32, (owners, 2 * cap), 1)
    both = jnp.concatenate([labels, labels], axis=1)
    mine = jnp.where((lane >= cap) == (core == 1), both, -1)[:, None, :]
    dma = pltpu.SemaphoreType.DMA
    out = pl.pallas_call(
        lambda *refs: exchange_kernel(owners, *refs),
        out_shape=jax.ShapeDtypeStruct((chips, 2 * cap), jnp.float32),
        in_specs=[pl.BlockSpec(memory_space=pl.ANY), pl.BlockSpec(memory_space=pltpu.VMEM)],
        out_specs=pl.BlockSpec(memory_space=pltpu.VMEM),
        scratch_shapes=[
            pltpu.VMEM((rows_here, width), jnp.bfloat16),
            pltpu.VMEM((owners, cap, width), jnp.bfloat16),
            pltpu.VMEM((rows_here, width), jnp.bfloat16),
            pltpu.VMEM((owners, 1, 2 * cap), jnp.int32),
            pltpu.VMEM((chips, 1, 2 * cap), jnp.int32),
            pltpu.VMEM((rows_here, 2 * cap), jnp.int32),
            pltpu.VMEM((rows_here, 2 * cap), jnp.float32),
            pltpu.VMEM((chips, 1, 2 * cap), jnp.float32),
            pltpu.VMEM((chips, 1, 2 * cap), jnp.float32),
            pltpu.VMEM((owners, 1, 2 * cap), jnp.float32),
            dma, dma((2,)),
            dma((owners,)), dma((owners,)), dma((owners,)), dma((owners,)), dma((owners,)), dma((owners,)),
        ],
        compiler_params=pltpu.CompilerParams(
            collective_id=0, has_side_effects=True, vmem_limit_bytes=48 << 20),
        cost_estimate=pl.CostEstimate(
            flops=2 * rows_here * rows_here * width, bytes_accessed=4 * rows_here * width, transcendentals=0),
    )(embeddings, mine)
    return out.reshape(rows_here)


def solution(mesh):
    return jax.shard_map(
        on_device,
        mesh=mesh,
        in_specs=(P(("parts", OWNER), None), P(("parts", OWNER)), P(("parts", OWNER), None)),
        out_specs=P(("parts", OWNER)),
        check_vma=False,
    )
```

```python
import math

import jax
import jax.numpy as jnp
from jax import lax
from jax.experimental import pallas as pl
from jax.experimental.pallas import tpu as pltpu
from jax.sharding import PartitionSpec as P

NEAR = 4
GROUP = 4
OWNER = "owner"


def exchange_kernel(
    owners, lengths, emb_hbm, cluster_ref, out_ref,
    emb_v, land, units, lab_out, lab_land, labrow, labcol, rowacc, colbest, res_out, res_land,
    load_sem, self_sem, send_sem, recv_sem, lab_send, lab_recv, res_send, res_recv, round_sem,
):
    chips = owners // 2
    far = chips // 2
    cap = land.shape[1]
    width = land.shape[2]
    tile = 4 * cap
    half_tile = 2 * cap
    span = GROUP * tile
    last = far - 1
    me = lax.axis_index(OWNER)
    core = lax.rem(me, 2)
    chip = me // 2
    partner = chip * 2 + 1 - core
    opposite = lax.rem(chip + far, chips)

    def distance(t):
        if isinstance(t, int):
            return t + 2 if t < NEAR - 1 else 1 if t == last else far - 1 - (t - NEAR)
        raise TypeError

    def on_right(k):
        return lax.rem(chip + k, chips)

    def on_left(k):
        return lax.rem(chip + chips - k, chips)

    load = pltpu.make_async_copy(emb_hbm, emb_v, load_sem)
    load.start()

    barrier = pltpu.get_barrier_semaphore()

    def greet(k, _):
        for c in range(2):
            pl.semaphore_signal(barrier, inc=1, device_id={OWNER: on_right(k) * 2 + c})
            pl.semaphore_signal(barrier, inc=1, device_id={OWNER: on_left(k) * 2 + c})
        return 0

    pl.semaphore_signal(barrier, inc=1, device_id={OWNER: partner})
    lax.fori_loop(1, NEAR + 1, greet, 0)

    lane = lax.broadcasted_iota(jnp.int32, (1, half_tile), 1)
    slot_of = jnp.where(lane < cap, lane, lane - cap)
    for m in range(chips):
        limit = jnp.where(lane < cap, lengths[0, 2 * m], lengths[0, 2 * m + 1])
        lab_out[m] = jnp.where(slot_of < limit, cluster_ref[m:m + 1, :], -1)
    labcol[...] = jnp.full_like(labcol, -2)
    rowacc[...] = jnp.full_like(rowacc, -1.0)

    load.wait()
    pl.semaphore_wait(barrier, 4 * NEAR + 1)

    def block_copy(dest, slot, land_slot):
        return pltpu.make_async_remote_copy(
            src_ref=emb_v.at[pl.ds(pl.multiple_of(dest * cap, cap), cap)],
            dst_ref=land.at[land_slot],
            send_sem=send_sem.at[slot],
            recv_sem=recv_sem.at[land_slot],
            device_id={OWNER: dest},
        )

    def label_copy(dest, slot, land_slot):
        return pltpu.make_async_remote_copy(
            src_ref=lab_out.at[dest // 2],
            dst_ref=lab_land.at[land_slot],
            send_sem=lab_send.at[slot],
            recv_sem=lab_recv.at[land_slot],
            device_id={OWNER: dest},
        )

    def start(dest, slot, land_slot):
        label_copy(dest, slot, land_slot).start()
        block_copy(dest, slot, land_slot).start()

    def send_tile(t, k):
        for c in range(2):
            start(on_right(k) * 2 + c, t * 4 + c, t * 4 + core)
            start(on_left(k) * 2 + c, t * 4 + 2 + c, t * 4 + 2 + core)

    own = NEAR - 1
    keep = pltpu.make_async_copy(
        emb_v.at[pl.ds(pl.multiple_of(me * cap, cap), cap)], land.at[4 * own + core], self_sem.at[0])
    keep_lab = pltpu.make_async_copy(lab_out.at[chip], lab_land.at[4 * own + core], self_sem.at[1])
    keep.start()
    keep_lab.start()
    start(partner, 4 * own, 4 * own + core)
    for t in range(NEAR - 1):
        send_tile(t, distance(t))

    for r in range(far // NEAR - 1):
        pl.semaphore_signal(round_sem.at[r, 0], inc=1, device_id={OWNER: on_right(NEAR) * 2 + core})
        pl.semaphore_signal(round_sem.at[r, 1], inc=1, device_id={OWNER: on_left(NEAR) * 2 + core})
        for i in range(2):
            pl.semaphore_wait(round_sem.at[r, i], 1)

    for c in range(2):
        start(opposite * 2 + c, 4 * own + 2 + c, 4 * own + 2 + core)

    def issue(t, _):
        send_tile(t, far - 1 - (t - NEAR))
        return 0

    lax.fori_loop(NEAR, last, issue, 0)
    send_tile(last, 1)

    def take_labels(t):
        for h in range(2):
            low, high = lab_land[4 * t + 2 * h], lab_land[4 * t + 2 * h + 1]
            low = jnp.where(core == 0, low, pltpu.roll(low, cap, 1))
            high = jnp.where(core == 0, pltpu.roll(high, cap, 1), high)
            row = jnp.where(lane < cap, low, high)
            labrow[2 * t + h] = row
            column = jnp.transpose(jnp.broadcast_to(row, (half_tile, half_tile)))
            labcol[pl.ds(pl.multiple_of(t * tile + h * half_tile, half_tile), half_tile), :] = jnp.where(
                column < 0, -2, column)

    def take_rows(t):
        values = land[pl.ds(4 * t, 4)].reshape(tile, width).astype(jnp.float32)
        factor = lax.rsqrt(jnp.mean(values * values, axis=-1, keepdims=True) + 1e-06) / math.sqrt(width)
        units[pl.ds(pl.multiple_of(t * tile, tile), tile), :] = (values * factor).astype(jnp.bfloat16)

    def group(t, g, running, diagonal):
        rows = pl.ds(pl.multiple_of(g * span, span), span)
        old = units[rows, :]
        fresh = units[pl.ds(pl.multiple_of(t * tile, tile), tile), :]
        sim = lax.dot_general(
            old, fresh, (((1,), (1,)), ((), ())), preferred_element_type=jnp.float32)
        col = labcol[rows, :]
        acc = rowacc[rows, :]
        out = []
        for h in range(2):
            part = sim[:, h * half_tile:(h + 1) * half_tile]
            same = col == labrow[2 * t + h]
            if diagonal:
                i = g * span + lax.broadcasted_iota(jnp.int32, part.shape, 0)
                j = t * tile + h * half_tile + lax.broadcasted_iota(jnp.int32, part.shape, 1)
                same = same & (i != j)
            part = jnp.where(same, part, -1.0)
            acc = jnp.maximum(acc, part)
            out.append(jnp.maximum(running[h], jnp.max(part, axis=0, keepdims=True)))
        return acc, tuple(out)

    def keep_group(t, g, running, diagonal):
        acc, running = group(t, g, running, diagonal)
        rowacc[pl.ds(pl.multiple_of(g * span, span), span), :] = acc
        return running

    floor = (jnp.full((1, half_tile), -1.0, jnp.float32),) * 2

    def labels_in(slot):
        label_copy(me, slot, slot).wait_recv()

    def rows_in(slot):
        block_copy(me, slot, slot).wait_recv()

    def take_tile(t, others):
        for s in others:
            labels_in(4 * t + s)
        take_labels(t)
        for s in others:
            rows_in(4 * t + s)
        take_rows(t)

    def whole_tile(t, others=(0, 1, 2, 3)):
        take_tile(t, others)
        running = lax.fori_loop(0, t // GROUP, lambda g, r: keep_group(t, g, r, False), floor)
        running = keep_group(t, t // GROUP, running, True)
        for h in range(2):
            colbest[2 * t + h] = running[h]

    def result_copy(row, dest, slot):
        return pltpu.make_async_remote_copy(
            src_ref=res_out.at[row],
            dst_ref=res_land.at[me],
            send_sem=res_send.at[slot],
            recv_sem=res_recv.at[me],
            device_id={OWNER: dest},
        )

    def give(t, k):
        for c in range(2):
            result_copy(2 * t, on_left(k) * 2 + c, t * 4 + c).start()
            result_copy(2 * t + 1, on_right(k) * 2 + c, t * 4 + 2 + c).start()

    def step(t, _):
        whole_tile(t)
        return 0

    lax.fori_loop(0, own, step, 0)
    keep.wait()
    keep_lab.wait()
    whole_tile(own, (1 - core, 2, 3))
    lax.fori_loop(NEAR, last, step, 0)

    take_tile(last, (0, 1, 2, 3))
    square = (half_tile, half_tile)
    on_diagonal = lax.broadcasted_iota(jnp.int32, square, 0) == lax.broadcasted_iota(jnp.int32, square, 1)
    running = floor
    for g in range(far // GROUP):
        acc, running = group(last, g, running, g == last // GROUP)
        for n in range(2 * GROUP):
            i = 2 * GROUP * g + n
            best = jnp.max(acc[n * half_tile:(n + 1) * half_tile, :], axis=1, keepdims=True)
            row = jnp.max(jnp.where(on_diagonal, best, -1.0), axis=0, keepdims=True)
            old = running[n % 2] if i // 2 == last else colbest[i]
            res_out[i] = jnp.maximum(old, row)
        if g == own // GROUP:
            for c in range(2):
                result_copy(2 * own + 1, opposite * 2 + c, 4 * own + 2 + c).start()
            result_copy(2 * own, partner, 4 * own).start()
            res_land[me] = res_out[2 * own]
        for t in range(GROUP * g, GROUP * (g + 1)):
            if t != own:
                give(t, distance(t))

    def back(i, _):
        s = lax.rem(me + i, owners)
        pltpu.make_async_remote_copy(
            src_ref=res_out.at[0], dst_ref=res_land.at[s], send_sem=res_send.at[0],
            recv_sem=res_recv.at[s], device_id={OWNER: s},
        ).wait_recv()
        return 0

    lax.fori_loop(1, owners, back, 0)

    for k in range(chips):
        low, high = res_land[2 * k], res_land[2 * k + 1]
        low = jnp.where(core == 0, low, pltpu.roll(low, cap, 1))
        high = jnp.where(core == 0, pltpu.roll(high, cap, 1), high)
        out_ref[k:k + 1, :] = jnp.where(lane < cap, low, high)

    def sent(slot, _):
        block_copy(me, slot, slot).wait_send()
        label_copy(me, slot, slot).wait_send()
        result_copy(0, me, slot).wait_send()
        return 0

    lax.fori_loop(0, 4 * own + 1, sent, 0)
    lax.fori_loop(4 * own + 2, owners, sent, 0)


def on_device(embeddings, cluster, lengths):
    owners = lax.axis_size(OWNER)
    rows_here, width = embeddings.shape
    cap = rows_here // owners
    chips = owners // 2
    dma = pltpu.SemaphoreType.DMA
    out = pl.pallas_call(
        lambda *refs: exchange_kernel(owners, *refs),
        out_shape=jax.ShapeDtypeStruct((chips, 2 * cap), jnp.float32),
        in_specs=[
            pl.BlockSpec(memory_space=pltpu.SMEM),
            pl.BlockSpec(memory_space=pltpu.HBM),
            pl.BlockSpec(memory_space=pltpu.VMEM),
        ],
        out_specs=pl.BlockSpec(memory_space=pltpu.VMEM),
        scratch_shapes=[
            pltpu.VMEM((rows_here, width), jnp.bfloat16),
            pltpu.VMEM((owners, cap, width), jnp.bfloat16),
            pltpu.VMEM((rows_here, width), jnp.bfloat16),
            pltpu.VMEM((chips, 1, 2 * cap), jnp.int32),
            pltpu.VMEM((owners, 1, 2 * cap), jnp.int32),
            pltpu.VMEM((chips, 1, 2 * cap), jnp.int32),
            pltpu.VMEM((rows_here, 2 * cap), jnp.int32),
            pltpu.VMEM((rows_here, 2 * cap), jnp.float32),
            pltpu.VMEM((chips, 1, 2 * cap), jnp.float32),
            pltpu.VMEM((chips, 1, 2 * cap), jnp.float32),
            pltpu.VMEM((owners, 1, 2 * cap), jnp.float32),
            dma, dma((2,)),
            dma((owners,)), dma((owners,)), dma((owners,)), dma((owners,)), dma((owners,)), dma((owners,)),
            pltpu.SemaphoreType.REGULAR((chips // 2 // NEAR, 2)),
        ],
        compiler_params=pltpu.CompilerParams(
            collective_id=0, has_side_effects=True),
        cost_estimate=pl.CostEstimate(
            flops=2 * rows_here * rows_here * width, bytes_accessed=4 * rows_here * width, transcendentals=0),
    )(lengths, embeddings, cluster.reshape(chips, 2 * cap))
    return out.reshape(rows_here)


def solution(mesh):
    return jax.shard_map(
        on_device,
        mesh=mesh,
        in_specs=(P(("parts", OWNER), None), P(("parts", OWNER)), P(("parts", OWNER), None)),
        out_specs=P(("parts", OWNER)),
        check_vma=False,
    )
```

```python
import math

import jax
import jax.numpy as jnp
from jax import lax
from jax.experimental import pallas as pl
from jax.experimental.pallas import tpu as pltpu
from jax.sharding import PartitionSpec as P

NEAR = 4
GROUP = 4
OWNER = "owner"


def exchange_kernel(
    owners, lengths, emb_hbm, cluster_ref, out_ref,
    emb_v, land, units, lab_out, lab_land, labrow, labcol, rowacc, colbest, res_out, res_land,
    load_sem, self_sem, send_sem, recv_sem, lab_send, lab_recv, res_send, res_recv, round_sem,
):
    chips = owners // 2
    far = chips // 2
    cap = land.shape[1]
    width = land.shape[2]
    tile = 4 * cap
    half_tile = 2 * cap
    span = GROUP * tile
    last = far - 1
    me = lax.axis_index(OWNER)
    core = lax.rem(me, 2)
    chip = me // 2
    partner = chip * 2 + 1 - core
    opposite = lax.rem(chip + far, chips)

    def distance(t):
        return t + 1 if t < NEAR else far - (t - NEAR)

    def on_right(k):
        return lax.rem(chip + k, chips)

    def on_left(k):
        return lax.rem(chip + chips - k, chips)

    load = pltpu.make_async_copy(emb_hbm, emb_v, load_sem)
    load.start()

    barrier = pltpu.get_barrier_semaphore()

    neighbours = (on_right(1) * 2 + core, on_left(1) * 2 + core, partner)
    for neighbour in neighbours:
        pl.semaphore_signal(barrier, inc=1, device_id={OWNER: neighbour})

    def hear(r):
        for i, neighbour in enumerate(neighbours):
            pl.semaphore_signal(round_sem.at[r, i], inc=1, device_id={OWNER: neighbour})
        for i in range(3):
            pl.semaphore_wait(round_sem.at[r, i], 1)

    lane = lax.broadcasted_iota(jnp.int32, (1, half_tile), 1)
    slot_of = jnp.where(lane < cap, lane, lane - cap)
    for m in range(chips):
        limit = jnp.where(lane < cap, lengths[0, 2 * m], lengths[0, 2 * m + 1])
        row = jnp.where(slot_of < limit, cluster_ref[m:m + 1, :], -1)
        lab_out[2 * m] = row[:, :cap]
        lab_out[2 * m + 1] = row[:, cap:]
    labcol[...] = jnp.full_like(labcol, -2)
    rowacc[...] = jnp.full_like(rowacc, -1.0)

    load.wait()
    pl.semaphore_wait(barrier, 3)

    def block_copy(dest, slot, land_slot):
        return pltpu.make_async_remote_copy(
            src_ref=emb_v.at[pl.ds(pl.multiple_of(dest * cap, cap), cap)],
            dst_ref=land.at[land_slot],
            send_sem=send_sem.at[slot],
            recv_sem=recv_sem.at[land_slot],
            device_id={OWNER: dest},
        )

    def label_copy(dest, slot, land_slot):
        return pltpu.make_async_remote_copy(
            src_ref=lab_out.at[dest],
            dst_ref=lab_land.at[land_slot],
            send_sem=lab_send.at[slot],
            recv_sem=lab_recv.at[land_slot],
            device_id={OWNER: dest},
        )

    def start(dest, slot, land_slot):
        label_copy(dest, slot, land_slot).start()
        block_copy(dest, slot, land_slot).start()

    def send_tile(t, k):
        for c in range(2):
            start(on_right(k) * 2 + c, t * 4 + c, t * 4 + core)
            start(on_left(k) * 2 + c, t * 4 + 2 + c, t * 4 + 2 + core)

    own = NEAR
    keep = pltpu.make_async_copy(
        emb_v.at[pl.ds(pl.multiple_of(me * cap, cap), cap)], land.at[4 * own + core], self_sem.at[0])
    keep_lab = pltpu.make_async_copy(lab_out.at[me], lab_land.at[4 * own + core], self_sem.at[1])
    keep.start()
    keep_lab.start()
    start(partner, 4 * own, 4 * own + core)
    for t in range(NEAR):
        hear(t)
        send_tile(t, distance(t))
    for r in range(NEAR, far):
        hear(r)

    for c in range(2):
        start(opposite * 2 + c, 4 * own + 2 + c, 4 * own + 2 + core)

    def issue(t, _):
        send_tile(t, far - (t - NEAR))
        return 0

    lax.fori_loop(NEAR + 1, far, issue, 0)

    def take_labels(t):
        for h in range(2):
            row = jnp.concatenate([lab_land[4 * t + 2 * h], lab_land[4 * t + 2 * h + 1]], axis=1)
            labrow[2 * t + h] = row
            column = jnp.transpose(jnp.broadcast_to(row, (half_tile, half_tile)))
            labcol[pl.ds(pl.multiple_of(t * tile + h * half_tile, half_tile), half_tile), :] = jnp.where(
                column < 0, -2, column)

    def take_rows(t):
        values = land[pl.ds(4 * t, 4)].reshape(tile, width).astype(jnp.float32)
        factor = lax.rsqrt(jnp.mean(values * values, axis=-1, keepdims=True) + 1e-06) / math.sqrt(width)
        units[pl.ds(pl.multiple_of(t * tile, tile), tile), :] = (values * factor).astype(jnp.bfloat16)

    def group(t, g, running, diagonal):
        rows = pl.ds(pl.multiple_of(g * span, span), span)
        old = units[rows, :]
        fresh = units[pl.ds(pl.multiple_of(t * tile, tile), tile), :]
        sim = lax.dot_general(
            old, fresh, (((1,), (1,)), ((), ())), preferred_element_type=jnp.float32)
        col = labcol[rows, :]
        acc = rowacc[rows, :]
        out = []
        for h in range(2):
            part = sim[:, h * half_tile:(h + 1) * half_tile]
            same = col == labrow[2 * t + h]
            if diagonal:
                i = g * span + lax.broadcasted_iota(jnp.int32, part.shape, 0)
                j = t * tile + h * half_tile + lax.broadcasted_iota(jnp.int32, part.shape, 1)
                same = same & (i != j)
            part = jnp.where(same, part, -1.0)
            acc = jnp.maximum(acc, part)
            out.append(jnp.maximum(running[h], jnp.max(part, axis=0, keepdims=True)))
        return acc, tuple(out)

    def keep_group(t, g, running, diagonal):
        acc, running = group(t, g, running, diagonal)
        rowacc[pl.ds(pl.multiple_of(g * span, span), span), :] = acc
        return running

    floor = (jnp.full((1, half_tile), -1.0, jnp.float32),) * 2

    def labels_in(slot):
        label_copy(me, slot, slot).wait_recv()

    def rows_in(slot):
        block_copy(me, slot, slot).wait_recv()

    def take_tile(t, others):
        for s in others:
            labels_in(4 * t + s)
        take_labels(t)
        for s in others:
            rows_in(4 * t + s)
        take_rows(t)

    def whole_tile(t, others=(0, 1, 2, 3)):
        take_tile(t, others)
        running = lax.fori_loop(0, t // GROUP, lambda g, r: keep_group(t, g, r, False), floor)
        running = keep_group(t, t // GROUP, running, True)
        for h in range(2):
            colbest[2 * t + h] = running[h]

    def result_copy(row, dest, slot):
        return pltpu.make_async_remote_copy(
            src_ref=res_out.at[row],
            dst_ref=res_land.at[me],
            send_sem=res_send.at[slot],
            recv_sem=res_recv.at[me],
            device_id={OWNER: dest},
        )

    def give(t, k):
        for c in range(2):
            result_copy(2 * t, on_left(k) * 2 + c, t * 4 + c).start()
            result_copy(2 * t + 1, on_right(k) * 2 + c, t * 4 + 2 + c).start()

    def step(t, _):
        whole_tile(t)
        return 0

    lax.fori_loop(0, own, step, 0)
    keep.wait()
    keep_lab.wait()
    whole_tile(own, (1 - core, 2, 3))
    lax.fori_loop(own + 1, last, step, 0)

    take_tile(last, (0, 1, 2, 3))
    square = (half_tile, half_tile)
    on_diagonal = lax.broadcasted_iota(jnp.int32, square, 0) == lax.broadcasted_iota(jnp.int32, square, 1)
    running = floor
    groups = far // GROUP
    for n in range(groups):
        g = (own // GROUP + n) % groups
        acc, running = group(last, g, running, g == last // GROUP)
        for m in range(2 * GROUP):
            i = 2 * GROUP * g + m
            best = jnp.max(acc[m * half_tile:(m + 1) * half_tile, :], axis=1, keepdims=True)
            row = jnp.max(jnp.where(on_diagonal, best, -1.0), axis=0, keepdims=True)
            if i // 2 == last:
                colbest[i] = row
            else:
                res_out[i] = jnp.maximum(colbest[i], row)
        if g == own // GROUP:
            for c in range(2):
                result_copy(2 * own + 1, opposite * 2 + c, 4 * own + 2 + c).start()
            result_copy(2 * own, partner, 4 * own).start()
            res_land[me] = res_out[2 * own]
        for t in range(GROUP * g, GROUP * (g + 1)):
            if t not in (own, last):
                give(t, distance(t))
    for h in range(2):
        res_out[2 * last + h] = jnp.maximum(colbest[2 * last + h], running[h])
    give(last, distance(last))

    def back(i, _):
        s = lax.rem(me + i, owners)
        pltpu.make_async_remote_copy(
            src_ref=res_out.at[0], dst_ref=res_land.at[s], send_sem=res_send.at[0],
            recv_sem=res_recv.at[s], device_id={OWNER: s},
        ).wait_recv()
        return 0

    lax.fori_loop(1, owners, back, 0)

    for k in range(chips):
        low, high = res_land[2 * k], res_land[2 * k + 1]
        low = jnp.where(core == 0, low, pltpu.roll(low, cap, 1))
        high = jnp.where(core == 0, pltpu.roll(high, cap, 1), high)
        out_ref[k:k + 1, :] = jnp.where(lane < cap, low, high)

    def sent(slot, _):
        block_copy(me, slot, slot).wait_send()
        label_copy(me, slot, slot).wait_send()
        result_copy(0, me, slot).wait_send()
        return 0

    lax.fori_loop(0, 4 * own + 1, sent, 0)
    lax.fori_loop(4 * own + 2, owners, sent, 0)


def on_device(embeddings, cluster, lengths):
    owners = lax.axis_size(OWNER)
    rows_here, width = embeddings.shape
    cap = rows_here // owners
    chips = owners // 2
    dma = pltpu.SemaphoreType.DMA
    out = pl.pallas_call(
        lambda *refs: exchange_kernel(owners, *refs),
        out_shape=jax.ShapeDtypeStruct((chips, 2 * cap), jnp.float32),
        in_specs=[
            pl.BlockSpec(memory_space=pltpu.SMEM),
            pl.BlockSpec(memory_space=pltpu.HBM),
            pl.BlockSpec(memory_space=pltpu.VMEM),
        ],
        out_specs=pl.BlockSpec(memory_space=pltpu.VMEM),
        scratch_shapes=[
            pltpu.VMEM((rows_here, width), jnp.bfloat16),
            pltpu.VMEM((owners, cap, width), jnp.bfloat16),
            pltpu.VMEM((rows_here, width), jnp.bfloat16),
            pltpu.VMEM((owners, 1, cap), jnp.int32),
            pltpu.VMEM((owners, 1, cap), jnp.int32),
            pltpu.VMEM((chips, 1, 2 * cap), jnp.int32),
            pltpu.VMEM((rows_here, 2 * cap), jnp.int32),
            pltpu.VMEM((rows_here, 2 * cap), jnp.float32),
            pltpu.VMEM((chips, 1, 2 * cap), jnp.float32),
            pltpu.VMEM((chips, 1, 2 * cap), jnp.float32),
            pltpu.VMEM((owners, 1, 2 * cap), jnp.float32),
            dma, dma((2,)),
            dma((owners,)), dma((owners,)), dma((owners,)), dma((owners,)), dma((owners,)), dma((owners,)),
            pltpu.SemaphoreType.REGULAR((chips // 2, 3)),
        ],
        compiler_params=pltpu.CompilerParams(
            collective_id=0, has_side_effects=True),
        cost_estimate=pl.CostEstimate(
            flops=2 * rows_here * rows_here * width, bytes_accessed=4 * rows_here * width, transcendentals=0),
    )(lengths, embeddings, cluster.reshape(chips, 2 * cap))
    return out.reshape(rows_here)


def solution(mesh):
    return jax.shard_map(
        on_device,
        mesh=mesh,
        in_specs=(P(("parts", OWNER), None), P(("parts", OWNER)), P(("parts", OWNER), None)),
        out_specs=P(("parts", OWNER)),
        check_vma=False,
    )
```

```python
import math

import jax
import jax.numpy as jnp
from jax import lax
from jax.experimental import pallas as pl
from jax.experimental.pallas import tpu as pltpu
from jax.sharding import PartitionSpec as P

NEAR = 4
GROUP = 4
OWNER = "owner"


def exchange_kernel(
    owners, lengths, emb_hbm, cluster_ref, out_ref,
    emb_v, land, units, lab_out, lab_land, labrow, labcol, rowacc, colbest, res_out, res_land,
    load_sem, self_sem, send_sem, recv_sem, lab_send, lab_recv, res_send, res_recv, round_sem,
):
    chips = owners // 2
    far = chips // 2
    cap = land.shape[1]
    width = land.shape[2]
    tile = 4 * cap
    half_tile = 2 * cap
    span = GROUP * tile
    last = far - 1
    me = lax.axis_index(OWNER)
    core = lax.rem(me, 2)
    chip = me // 2
    partner = chip * 2 + 1 - core
    opposite = lax.rem(chip + far, chips)

    def distance(t):
        return t + 1 if t < NEAR else far - (t - NEAR)

    def on_right(k):
        return lax.rem(chip + k, chips)

    def on_left(k):
        return lax.rem(chip + chips - k, chips)

    load = pltpu.make_async_copy(emb_hbm, emb_v, load_sem)
    load.start()

    barrier = pltpu.get_barrier_semaphore()

    for neighbour in (on_right(1), on_left(1)):
        for c in range(2):
            pl.semaphore_signal(barrier, inc=1, device_id={OWNER: neighbour * 2 + c})
    pl.semaphore_signal(barrier, inc=1, device_id={OWNER: partner})

    def hear(r):
        for i, neighbour in enumerate((on_right(1), on_left(1))):
            pl.semaphore_signal(round_sem.at[r, i], inc=1, device_id={OWNER: neighbour * 2 + core})
        for i in range(2):
            pl.semaphore_wait(round_sem.at[r, i], 1)

    lane = lax.broadcasted_iota(jnp.int32, (1, half_tile), 1)
    slot_of = jnp.where(lane < cap, lane, lane - cap)
    for m in range(chips):
        limit = jnp.where(lane < cap, lengths[0, 2 * m], lengths[0, 2 * m + 1])
        row = jnp.where(slot_of < limit, cluster_ref[m:m + 1, :], -1)
        lab_out[2 * m] = row[:, :cap]
        lab_out[2 * m + 1] = row[:, cap:]
    labcol[...] = jnp.full_like(labcol, -2)
    rowacc[...] = jnp.full_like(rowacc, -1.0)

    load.wait()
    pl.semaphore_wait(barrier, 5)

    def block_copy(dest, slot, land_slot):
        return pltpu.make_async_remote_copy(
            src_ref=emb_v.at[pl.ds(pl.multiple_of(dest * cap, cap), cap)],
            dst_ref=land.at[land_slot],
            send_sem=send_sem.at[slot],
            recv_sem=recv_sem.at[land_slot],
            device_id={OWNER: dest},
        )

    def label_copy(dest, slot, land_slot):
        return pltpu.make_async_remote_copy(
            src_ref=lab_out.at[dest],
            dst_ref=lab_land.at[land_slot],
            send_sem=lab_send.at[slot],
            recv_sem=lab_recv.at[land_slot],
            device_id={OWNER: dest},
        )

    def start(dest, slot, land_slot):
        label_copy(dest, slot, land_slot).start()
        block_copy(dest, slot, land_slot).start()

    def send_tile(t, k):
        for c in range(2):
            start(on_right(k) * 2 + c, t * 4 + c, t * 4 + core)
            start(on_left(k) * 2 + c, t * 4 + 2 + c, t * 4 + 2 + core)

    own = NEAR
    keep = pltpu.make_async_copy(
        emb_v.at[pl.ds(pl.multiple_of(me * cap, cap), cap)], land.at[4 * own + core], self_sem.at[0])
    keep_lab = pltpu.make_async_copy(lab_out.at[me], lab_land.at[4 * own + core], self_sem.at[1])
    keep.start()
    keep_lab.start()
    start(partner, 4 * own, 4 * own + core)
    for t in range(NEAR):
        if t > 0:
            hear(t - 1)
        send_tile(t, distance(t))
    for r in range(NEAR - 1, far - 1):
        hear(r)

    for c in range(2):
        start(opposite * 2 + c, 4 * own + 2 + c, 4 * own + 2 + core)

    def issue(t, _):
        send_tile(t, far - (t - NEAR))
        return 0

    lax.fori_loop(NEAR + 1, far, issue, 0)

    def take_labels(t):
        for h in range(2):
            row = jnp.concatenate([lab_land[4 * t + 2 * h], lab_land[4 * t + 2 * h + 1]], axis=1)
            labrow[2 * t + h] = row
            column = jnp.transpose(jnp.broadcast_to(row, (half_tile, half_tile)))
            labcol[pl.ds(pl.multiple_of(t * tile + h * half_tile, half_tile), half_tile), :] = jnp.where(
                column < 0, -2, column)

    def take_rows(t):
        values = land[pl.ds(4 * t, 4)].reshape(tile, width).astype(jnp.float32)
        factor = lax.rsqrt(jnp.mean(values * values, axis=-1, keepdims=True) + 1e-06) / math.sqrt(width)
        units[pl.ds(pl.multiple_of(t * tile, tile), tile), :] = (values * factor).astype(jnp.bfloat16)

    def group(t, g, running, diagonal):
        rows = pl.ds(pl.multiple_of(g * span, span), span)
        old = units[rows, :]
        fresh = units[pl.ds(pl.multiple_of(t * tile, tile), tile), :]
        sim = lax.dot_general(
            old, fresh, (((1,), (1,)), ((), ())), preferred_element_type=jnp.float32)
        col = labcol[rows, :]
        acc = rowacc[rows, :]
        out = []
        for h in range(2):
            part = sim[:, h * half_tile:(h + 1) * half_tile]
            same = col == labrow[2 * t + h]
            if diagonal:
                i = g * span + lax.broadcasted_iota(jnp.int32, part.shape, 0)
                j = t * tile + h * half_tile + lax.broadcasted_iota(jnp.int32, part.shape, 1)
                same = same & (i != j)
            part = jnp.where(same, part, -1.0)
            acc = jnp.maximum(acc, part)
            out.append(jnp.maximum(running[h], jnp.max(part, axis=0, keepdims=True)))
        return acc, tuple(out)

    def keep_group(t, g, running, diagonal):
        acc, running = group(t, g, running, diagonal)
        rowacc[pl.ds(pl.multiple_of(g * span, span), span), :] = acc
        return running

    floor = (jnp.full((1, half_tile), -1.0, jnp.float32),) * 2

    def labels_in(slot):
        label_copy(me, slot, slot).wait_recv()

    def rows_in(slot):
        block_copy(me, slot, slot).wait_recv()

    def take_tile(t, others):
        for s in others:
            labels_in(4 * t + s)
        take_labels(t)
        for s in others:
            rows_in(4 * t + s)
        take_rows(t)

    def whole_tile(t, others=(0, 1, 2, 3)):
        take_tile(t, others)
        running = lax.fori_loop(0, t // GROUP, lambda g, r: keep_group(t, g, r, False), floor)
        running = keep_group(t, t // GROUP, running, True)
        for h in range(2):
            colbest[2 * t + h] = running[h]

    def result_copy(row, dest, slot):
        return pltpu.make_async_remote_copy(
            src_ref=res_out.at[row],
            dst_ref=res_land.at[me],
            send_sem=res_send.at[slot],
            recv_sem=res_recv.at[me],
            device_id={OWNER: dest},
        )

    def give(t, k):
        for c in range(2):
            result_copy(2 * t, on_left(k) * 2 + c, t * 4 + c).start()
            result_copy(2 * t + 1, on_right(k) * 2 + c, t * 4 + 2 + c).start()

    def step(t, _):
        whole_tile(t)
        return 0

    lax.fori_loop(0, own, step, 0)
    keep.wait()
    keep_lab.wait()
    whole_tile(own, (1 - core, 2, 3))
    lax.fori_loop(own + 1, last, step, 0)

    def left(slot, _):
        block_copy(me, slot, slot).wait_send()
        label_copy(me, slot, slot).wait_send()
        return 0

    lax.fori_loop(0, 4 * own + 1, left, 0)
    lax.fori_loop(4 * own + 2, 4 * last, left, 0)

    take_tile(last, (0, 1, 2, 3))
    square = (half_tile, half_tile)
    on_diagonal = lax.broadcasted_iota(jnp.int32, square, 0) == lax.broadcasted_iota(jnp.int32, square, 1)
    running = floor
    groups = far // GROUP
    for n in range(groups):
        g = (own // GROUP + n) % groups
        acc, running = group(last, g, running, g == last // GROUP)
        for m in range(2 * GROUP):
            i = 2 * GROUP * g + m
            best = jnp.max(acc[m * half_tile:(m + 1) * half_tile, :], axis=1, keepdims=True)
            row = jnp.max(jnp.where(on_diagonal, best, -1.0), axis=0, keepdims=True)
            if i // 2 == last:
                colbest[i] = row
            else:
                res_out[i] = jnp.maximum(colbest[i], row)
        if g == own // GROUP:
            for c in range(2):
                result_copy(2 * own + 1, opposite * 2 + c, 4 * own + 2 + c).start()
            result_copy(2 * own, partner, 4 * own).start()
            res_land[me] = res_out[2 * own]
        for t in range(GROUP * g, GROUP * (g + 1)):
            if t not in (own, last):
                give(t, distance(t))
    for h in range(2):
        res_out[2 * last + h] = jnp.maximum(colbest[2 * last + h], running[h])
    give(last, distance(last))

    def answered(slot, _):
        result_copy(0, me, slot).wait_send()
        return 0

    lax.fori_loop(4 * last, owners, left, 0)
    lax.fori_loop(0, 4 * own + 1, answered, 0)
    lax.fori_loop(4 * own + 2, owners, answered, 0)

    def back(i, _):
        s = lax.rem(me + i, owners)
        pltpu.make_async_remote_copy(
            src_ref=res_out.at[0], dst_ref=res_land.at[s], send_sem=res_send.at[0],
            recv_sem=res_recv.at[s], device_id={OWNER: s},
        ).wait_recv()
        return 0

    lax.fori_loop(1, owners, back, 0)

    for k in range(chips):
        low, high = res_land[2 * k], res_land[2 * k + 1]
        low = jnp.where(core == 0, low, pltpu.roll(low, cap, 1))
        high = jnp.where(core == 0, pltpu.roll(high, cap, 1), high)
        out_ref[k:k + 1, :] = jnp.where(lane < cap, low, high)


def on_device(embeddings, cluster, lengths):
    owners = lax.axis_size(OWNER)
    rows_here, width = embeddings.shape
    cap = rows_here // owners
    chips = owners // 2
    dma = pltpu.SemaphoreType.DMA
    out = pl.pallas_call(
        lambda *refs: exchange_kernel(owners, *refs),
        out_shape=jax.ShapeDtypeStruct((chips, 2 * cap), jnp.float32),
        in_specs=[
            pl.BlockSpec(memory_space=pltpu.SMEM),
            pl.BlockSpec(memory_space=pltpu.HBM),
            pl.BlockSpec(memory_space=pltpu.VMEM),
        ],
        out_specs=pl.BlockSpec(memory_space=pltpu.VMEM),
        scratch_shapes=[
            pltpu.VMEM((rows_here, width), jnp.bfloat16),
            pltpu.VMEM((owners, cap, width), jnp.bfloat16),
            pltpu.VMEM((rows_here, width), jnp.bfloat16),
            pltpu.VMEM((owners, 1, cap), jnp.int32),
            pltpu.VMEM((owners, 1, cap), jnp.int32),
            pltpu.VMEM((chips, 1, 2 * cap), jnp.int32),
            pltpu.VMEM((rows_here, 2 * cap), jnp.int32),
            pltpu.VMEM((rows_here, 2 * cap), jnp.float32),
            pltpu.VMEM((chips, 1, 2 * cap), jnp.float32),
            pltpu.VMEM((chips, 1, 2 * cap), jnp.float32),
            pltpu.VMEM((owners, 1, 2 * cap), jnp.float32),
            dma, dma((2,)),
            dma((owners,)), dma((owners,)), dma((owners,)), dma((owners,)), dma((owners,)), dma((owners,)),
            pltpu.SemaphoreType.REGULAR((chips // 2 - 1, 2)),
        ],
        compiler_params=pltpu.CompilerParams(
            collective_id=0, has_side_effects=True),
        cost_estimate=pl.CostEstimate(
            flops=2 * rows_here * rows_here * width, bytes_accessed=4 * rows_here * width, transcendentals=0),
    )(lengths, embeddings, cluster.reshape(chips, 2 * cap))
    return out.reshape(rows_here)


def solution(mesh):
    return jax.shard_map(
        on_device,
        mesh=mesh,
        in_specs=(P(("parts", OWNER), None), P(("parts", OWNER)), P(("parts", OWNER), None)),
        out_specs=P(("parts", OWNER)),
        check_vma=False,
    )
```

```python
import math

import jax
import jax.numpy as jnp
from jax import lax
from jax.experimental import pallas as pl
from jax.experimental.pallas import tpu as pltpu
from jax.sharding import PartitionSpec as P

NEAR = 4
GROUP = 4
OWNER = "owner"


def exchange_kernel(
    owners, lengths, emb_hbm, cluster_ref, out_ref,
    emb_v, first_v, land, units, lab_out, lab_other, lab_both, lab_land, labcol, rowacc, colbest, res_out, res_land,
    load_sem, self_sem, swap_sem, send_sem, recv_sem, lab_send, lab_recv, res_send, res_recv, round_sem,
):
    chips = owners // 2
    far = chips // 2
    cap = land.shape[1]
    width = land.shape[2]
    tile = 4 * cap
    half_tile = 2 * cap
    span = GROUP * tile
    last = far - 1
    me = lax.axis_index(OWNER)
    core = lax.rem(me, 2)
    chip = me // 2
    partner = chip * 2 + 1 - core
    opposite = lax.rem(chip + far, chips)

    def distance(t):
        return t + 1 if t < NEAR else far - (t - NEAR)

    def on_right(k):
        return lax.rem(chip + k, chips)

    def on_left(k):
        return lax.rem(chip + chips - k, chips)

    firsts = [
        pltpu.make_async_copy(
            emb_hbm.at[pl.ds(pl.multiple_of(there * half_tile, half_tile), half_tile)], first_v.at[i], load_sem.at[i])
        for i, there in enumerate((on_right(1), on_left(1)))
    ]
    for first in firsts:
        first.start()
    load = pltpu.make_async_copy(emb_hbm, emb_v, load_sem.at[2])
    load.start()

    barrier = pltpu.get_barrier_semaphore()

    for neighbour in (on_right(1), on_left(1)):
        for c in range(2):
            pl.semaphore_signal(barrier, inc=1, device_id={OWNER: neighbour * 2 + c})
    pl.semaphore_signal(barrier, inc=1, device_id={OWNER: partner})

    def hear(r):
        for i, neighbour in enumerate((on_right(1), on_left(1))):
            pl.semaphore_signal(round_sem.at[r, i], inc=1, device_id={OWNER: neighbour * 2 + core})
        for i in range(2):
            pl.semaphore_wait(round_sem.at[r, i], 1)

    lane = lax.broadcasted_iota(jnp.int32, (1, half_tile), 1)
    slot_of = jnp.where(lane < cap, lane, lane - cap)
    for m in range(chips):
        limit = jnp.where(lane < cap, lengths[0, 2 * m], lengths[0, 2 * m + 1])
        row = jnp.where(slot_of < limit, cluster_ref[m:m + 1, :], -1)
        lab_out[0, m] = row[:, :cap]
        lab_out[1, m] = row[:, cap:]

    pl.semaphore_wait(barrier, 5)
    for first in firsts:
        first.wait()

    def block_copy(dest, slot, land_slot):
        return pltpu.make_async_remote_copy(
            src_ref=emb_v.at[pl.ds(pl.multiple_of(dest * cap, cap), cap)],
            dst_ref=land.at[land_slot],
            send_sem=send_sem.at[slot],
            recv_sem=recv_sem.at[land_slot],
            device_id={OWNER: dest},
        )

    def label_copy(there, row):
        return pltpu.make_async_remote_copy(
            src_ref=lab_both.at[there],
            dst_ref=lab_land.at[row],
            send_sem=lab_send.at[row],
            recv_sem=lab_recv.at[row],
            device_id={OWNER: there * 2 + core},
        )

    def send_rows(t, k):
        for c in range(2):
            block_copy(on_right(k) * 2 + c, t * 4 + c, t * 4 + core).start()
            block_copy(on_left(k) * 2 + c, t * 4 + 2 + c, t * 4 + 2 + core).start()

    def send_labels(t, k):
        label_copy(on_right(k), 2 * t).start()
        label_copy(on_left(k), 2 * t + 1).start()

    own = NEAR
    for c in range(2):
        for i, there in enumerate((on_right(1), on_left(1))):
            pltpu.make_async_remote_copy(
                src_ref=first_v.at[i, pl.ds(c * cap, cap)],
                dst_ref=land.at[2 * i + core],
                send_sem=send_sem.at[2 * i + c],
                recv_sem=recv_sem.at[2 * i + core],
                device_id={OWNER: there * 2 + c},
            ).start()
    swap = pltpu.make_async_remote_copy(
        src_ref=lab_out.at[1 - core],
        dst_ref=lab_other,
        send_sem=swap_sem.at[0],
        recv_sem=swap_sem.at[1],
        device_id={OWNER: partner},
    )
    swap.start()
    load.wait()
    for t in range(1, NEAR):
        hear(t - 1)
        send_rows(t, distance(t))
    keep = pltpu.make_async_copy(
        emb_v.at[pl.ds(pl.multiple_of(me * cap, cap), cap)], land.at[4 * own + core], self_sem)
    keep.start()
    block_copy(partner, 4 * own, 4 * own + core).start()

    swap.wait()
    for m in range(chips):
        mine, other = lab_out[core, m], lab_other[m]
        lab_both[m] = jnp.concatenate(
            [jnp.where(core == 0, mine, other), jnp.where(core == 0, other, mine)], axis=1)
    lab_land[2 * own] = lab_both[chip]

    for r in range(NEAR - 1, far - 1):
        hear(r)
    for t in range(NEAR):
        send_labels(t, distance(t))

    label_copy(opposite, 2 * own + 1).start()
    for c in range(2):
        block_copy(opposite * 2 + c, 4 * own + 2 + c, 4 * own + 2 + core).start()

    def issue(t, _):
        send_labels(t, far - (t - NEAR))
        send_rows(t, far - (t - NEAR))
        return 0

    lax.fori_loop(NEAR + 1, far, issue, 0)

    labcol[...] = jnp.full_like(labcol, -2)
    rowacc[...] = jnp.full_like(rowacc, -1.0)

    def take_labels(t):
        for h in range(2):
            row = lab_land[2 * t + h]
            column = jnp.transpose(jnp.broadcast_to(row, (half_tile, half_tile)))
            labcol[pl.ds(pl.multiple_of(t * tile + h * half_tile, half_tile), half_tile), :] = jnp.where(
                column < 0, -2, column)

    def take_rows(t):
        values = land[pl.ds(4 * t, 4)].reshape(tile, width).astype(jnp.float32)
        factor = lax.rsqrt(jnp.mean(values * values, axis=-1, keepdims=True) + 1e-06) / math.sqrt(width)
        units[pl.ds(pl.multiple_of(t * tile, tile), tile), :] = (values * factor).astype(jnp.bfloat16)

    def group(t, g, running, diagonal):
        rows = pl.ds(pl.multiple_of(g * span, span), span)
        old = units[rows, :]
        fresh = units[pl.ds(pl.multiple_of(t * tile, tile), tile), :]
        sim = lax.dot_general(
            old, fresh, (((1,), (1,)), ((), ())), preferred_element_type=jnp.float32)
        col = labcol[rows, :]
        acc = rowacc[rows, :]
        out = []
        for h in range(2):
            part = sim[:, h * half_tile:(h + 1) * half_tile]
            same = col == lab_land[2 * t + h]
            if diagonal:
                i = g * span + lax.broadcasted_iota(jnp.int32, part.shape, 0)
                j = t * tile + h * half_tile + lax.broadcasted_iota(jnp.int32, part.shape, 1)
                same = same & (i != j)
            part = jnp.where(same, part, -1.0)
            acc = jnp.maximum(acc, part)
            out.append(jnp.maximum(running[h], jnp.max(part, axis=0, keepdims=True)))
        return acc, tuple(out)

    def keep_group(t, g, running, diagonal):
        acc, running = group(t, g, running, diagonal)
        rowacc[pl.ds(pl.multiple_of(g * span, span), span), :] = acc
        return running

    floor = (jnp.full((1, half_tile), -1.0, jnp.float32),) * 2

    def labels_in(row):
        label_copy(chip, row).wait_recv()

    def rows_in(slot):
        block_copy(me, slot, slot).wait_recv()

    def take_tile(t, others, halves):
        for h in halves:
            labels_in(2 * t + h)
        take_labels(t)
        for s in others:
            rows_in(4 * t + s)
        take_rows(t)

    def whole_tile(t, others=(0, 1, 2, 3), halves=(0, 1)):
        take_tile(t, others, halves)
        running = lax.fori_loop(0, t // GROUP, lambda g, r: keep_group(t, g, r, False), floor)
        running = keep_group(t, t // GROUP, running, True)
        for h in range(2):
            colbest[2 * t + h] = running[h]

    def result_copy(row, dest, slot):
        return pltpu.make_async_remote_copy(
            src_ref=res_out.at[row],
            dst_ref=res_land.at[me],
            send_sem=res_send.at[slot],
            recv_sem=res_recv.at[me],
            device_id={OWNER: dest},
        )

    def give(t, k):
        for c in range(2):
            result_copy(2 * t, on_left(k) * 2 + c, t * 4 + c).start()
            result_copy(2 * t + 1, on_right(k) * 2 + c, t * 4 + 2 + c).start()

    def step(t, _):
        whole_tile(t)
        return 0

    lax.fori_loop(0, own, step, 0)
    keep.wait()
    whole_tile(own, (1 - core, 2, 3), (1,))
    lax.fori_loop(own + 1, last, step, 0)

    def left(slot, _):
        block_copy(me, slot, slot).wait_send()
        return 0

    def told(row, _):
        label_copy(chip, row).wait_send()
        return 0

    lax.fori_loop(0, 2 * own, told, 0)
    lax.fori_loop(2 * own + 1, chips, told, 0)

    lax.fori_loop(0, 4 * own + 1, left, 0)
    lax.fori_loop(4 * own + 2, 4 * last, left, 0)

    take_tile(last, (0, 1, 2, 3), (0, 1))
    square = (half_tile, half_tile)
    on_diagonal = lax.broadcasted_iota(jnp.int32, square, 0) == lax.broadcasted_iota(jnp.int32, square, 1)
    running = floor
    groups = far // GROUP
    for n in range(groups):
        g = (own // GROUP + n) % groups
        acc, running = group(last, g, running, g == last // GROUP)
        for m in range(2 * GROUP):
            i = 2 * GROUP * g + m
            best = jnp.max(acc[m * half_tile:(m + 1) * half_tile, :], axis=1, keepdims=True)
            row = jnp.max(jnp.where(on_diagonal, best, -1.0), axis=0, keepdims=True)
            if i // 2 == last:
                colbest[i] = row
            else:
                res_out[i] = jnp.maximum(colbest[i], row)
        if g == own // GROUP:
            for c in range(2):
                result_copy(2 * own + 1, opposite * 2 + c, 4 * own + 2 + c).start()
            result_copy(2 * own, partner, 4 * own).start()
            res_land[me] = res_out[2 * own]
        for t in range(GROUP * g, GROUP * (g + 1)):
            if t not in (own, last):
                give(t, distance(t))
    for h in range(2):
        res_out[2 * last + h] = jnp.maximum(colbest[2 * last + h], running[h])
    give(last, distance(last))

    def answered(slot, _):
        result_copy(0, me, slot).wait_send()
        return 0

    lax.fori_loop(4 * last, owners, left, 0)
    lax.fori_loop(0, 4 * own + 1, answered, 0)
    lax.fori_loop(4 * own + 2, owners, answered, 0)

    def back(i, _):
        s = lax.rem(me + i, owners)
        pltpu.make_async_remote_copy(
            src_ref=res_out.at[0], dst_ref=res_land.at[s], send_sem=res_send.at[0],
            recv_sem=res_recv.at[s], device_id={OWNER: s},
        ).wait_recv()
        return 0

    lax.fori_loop(1, owners, back, 0)

    for k in range(chips):
        low, high = res_land[2 * k], res_land[2 * k + 1]
        low = jnp.where(core == 0, low, pltpu.roll(low, cap, 1))
        high = jnp.where(core == 0, pltpu.roll(high, cap, 1), high)
        out_ref[k:k + 1, :] = jnp.where(lane < cap, low, high)


def on_device(embeddings, cluster, lengths):
    owners = lax.axis_size(OWNER)
    rows_here, width = embeddings.shape
    cap = rows_here // owners
    chips = owners // 2
    dma = pltpu.SemaphoreType.DMA
    out = pl.pallas_call(
        lambda *refs: exchange_kernel(owners, *refs),
        out_shape=jax.ShapeDtypeStruct((chips, 2 * cap), jnp.float32),
        in_specs=[
            pl.BlockSpec(memory_space=pltpu.SMEM),
            pl.BlockSpec(memory_space=pltpu.HBM),
            pl.BlockSpec(memory_space=pltpu.VMEM),
        ],
        out_specs=pl.BlockSpec(memory_space=pltpu.VMEM),
        scratch_shapes=[
            pltpu.VMEM((rows_here, width), jnp.bfloat16),
            pltpu.VMEM((2, 2 * cap, width), jnp.bfloat16),
            pltpu.VMEM((owners, cap, width), jnp.bfloat16),
            pltpu.VMEM((rows_here, width), jnp.bfloat16),
            pltpu.VMEM((2, chips, 1, cap), jnp.int32),
            pltpu.VMEM((chips, 1, cap), jnp.int32),
            pltpu.VMEM((chips, 1, 2 * cap), jnp.int32),
            pltpu.VMEM((chips, 1, 2 * cap), jnp.int32),
            pltpu.VMEM((rows_here, 2 * cap), jnp.int32),
            pltpu.VMEM((rows_here, 2 * cap), jnp.float32),
            pltpu.VMEM((chips, 1, 2 * cap), jnp.float32),
            pltpu.VMEM((chips, 1, 2 * cap), jnp.float32),
            pltpu.VMEM((owners, 1, 2 * cap), jnp.float32),
            dma((3,)), dma, dma((2,)),
            dma((owners,)), dma((owners,)), dma((chips,)), dma((chips,)), dma((owners,)), dma((owners,)),
            pltpu.SemaphoreType.REGULAR((chips // 2 - 1, 2)),
        ],
        compiler_params=pltpu.CompilerParams(
            collective_id=0, has_side_effects=True),
        cost_estimate=pl.CostEstimate(
            flops=2 * rows_here * rows_here * width, bytes_accessed=4 * rows_here * width, transcendentals=0),
    )(lengths, embeddings, cluster.reshape(chips, 2 * cap))
    return out.reshape(rows_here)


def solution(mesh):
    return jax.shard_map(
        on_device,
        mesh=mesh,
        in_specs=(P(("parts", OWNER), None), P(("parts", OWNER)), P(("parts", OWNER), None)),
        out_specs=P(("parts", OWNER)),
        check_vma=False,
    )
```

```python
import math

import jax
import jax.numpy as jnp
from jax import lax
from jax.experimental import pallas as pl
from jax.experimental.pallas import tpu as pltpu
from jax.sharding import PartitionSpec as P

NEAR = 3
GROUP = 4
OWNER = "owner"


def exchange_kernel(
    owners, lengths, emb_hbm, cluster_ref, out_ref,
    emb_v, first_v, land, units, lab_out, lab_other, lab_both, lab_land, labcol, rowacc, colbest, res_out, res_land,
    load_sem, self_sem, swap_sem, send_sem, recv_sem, lab_send, lab_recv, res_send, res_recv, round_sem,
):
    chips = owners // 2
    far = chips // 2
    cap = land.shape[1]
    width = land.shape[2]
    tile = 4 * cap
    half_tile = 2 * cap
    span = GROUP * tile
    last = far - 1
    me = lax.axis_index(OWNER)
    core = lax.rem(me, 2)
    chip = me // 2
    partner = chip * 2 + 1 - core
    opposite = lax.rem(chip + far, chips)

    def distance(t):
        return 1 if t == 0 else 2 if t == last else t + 2 if t < NEAR else far - (t - NEAR)

    def on_right(k):
        return lax.rem(chip + k, chips)

    def on_left(k):
        return lax.rem(chip + chips - k, chips)

    firsts = [
        pltpu.make_async_copy(
            emb_hbm.at[pl.ds(pl.multiple_of(there * half_tile, half_tile), half_tile)], first_v.at[i], load_sem.at[i])
        for i, there in enumerate((on_right(1), on_left(1)))
    ]
    for first in firsts:
        first.start()
    load = pltpu.make_async_copy(emb_hbm, emb_v, load_sem.at[2])
    load.start()

    barrier = pltpu.get_barrier_semaphore()

    for neighbour in (on_right(1), on_left(1)):
        for c in range(2):
            pl.semaphore_signal(barrier, inc=1, device_id={OWNER: neighbour * 2 + c})
    pl.semaphore_signal(barrier, inc=1, device_id={OWNER: partner})

    def hear(r):
        for i, neighbour in enumerate((on_right(1), on_left(1))):
            pl.semaphore_signal(round_sem.at[r, i], inc=1, device_id={OWNER: neighbour * 2 + core})
        for i in range(2):
            pl.semaphore_wait(round_sem.at[r, i], 1)

    lane = lax.broadcasted_iota(jnp.int32, (1, half_tile), 1)
    slot_of = jnp.where(lane < cap, lane, lane - cap)
    for m in range(chips):
        limit = jnp.where(lane < cap, lengths[0, 2 * m], lengths[0, 2 * m + 1])
        row = jnp.where(slot_of < limit, cluster_ref[m:m + 1, :], -1)
        lab_out[0, m] = row[:, :cap]
        lab_out[1, m] = row[:, cap:]

    pl.semaphore_wait(barrier, 5)
    for first in firsts:
        first.wait()

    def block_copy(dest, slot, land_slot):
        return pltpu.make_async_remote_copy(
            src_ref=emb_v.at[pl.ds(pl.multiple_of(dest * cap, cap), cap)],
            dst_ref=land.at[land_slot],
            send_sem=send_sem.at[slot],
            recv_sem=recv_sem.at[land_slot],
            device_id={OWNER: dest},
        )

    def label_copy(there, row):
        return pltpu.make_async_remote_copy(
            src_ref=lab_both.at[there],
            dst_ref=lab_land.at[row],
            send_sem=lab_send.at[row],
            recv_sem=lab_recv.at[row],
            device_id={OWNER: there * 2 + core},
        )

    def send_rows(t, k):
        for c in range(2):
            block_copy(on_right(k) * 2 + c, t * 4 + c, t * 4 + core).start()
            block_copy(on_left(k) * 2 + c, t * 4 + 2 + c, t * 4 + 2 + core).start()

    def send_labels(t, k):
        label_copy(on_right(k), 2 * t).start()
        label_copy(on_left(k), 2 * t + 1).start()

    own = NEAR
    for c in range(2):
        for i, there in enumerate((on_right(1), on_left(1))):
            pltpu.make_async_remote_copy(
                src_ref=first_v.at[i, pl.ds(c * cap, cap)],
                dst_ref=land.at[2 * i + core],
                send_sem=send_sem.at[2 * i + c],
                recv_sem=recv_sem.at[2 * i + core],
                device_id={OWNER: there * 2 + c},
            ).start()
    swap = pltpu.make_async_remote_copy(
        src_ref=lab_out.at[1 - core],
        dst_ref=lab_other,
        send_sem=swap_sem.at[0],
        recv_sem=swap_sem.at[1],
        device_id={OWNER: partner},
    )
    swap.start()
    load.wait()
    heard = 0
    for t in range(1, NEAR):
        for r in range(heard, distance(t) - 1):
            hear(r)
        heard = distance(t) - 1
        send_rows(t, distance(t))
    keep = pltpu.make_async_copy(
        emb_v.at[pl.ds(pl.multiple_of(me * cap, cap), cap)], land.at[4 * own + core], self_sem)
    keep.start()
    block_copy(partner, 4 * own, 4 * own + core).start()

    swap.wait()
    for m in range(chips):
        mine, other = lab_out[core, m], lab_other[m]
        lab_both[m] = jnp.concatenate(
            [jnp.where(core == 0, mine, other), jnp.where(core == 0, other, mine)], axis=1)
    lab_land[2 * own] = lab_both[chip]

    for r in range(heard, far - 1):
        hear(r)
    for t in range(NEAR):
        send_labels(t, distance(t))

    label_copy(opposite, 2 * own + 1).start()
    for c in range(2):
        block_copy(opposite * 2 + c, 4 * own + 2 + c, 4 * own + 2 + core).start()

    def issue(t, _):
        send_labels(t, far - (t - NEAR))
        send_rows(t, far - (t - NEAR))
        return 0

    lax.fori_loop(NEAR + 1, last, issue, 0)
    send_labels(last, distance(last))
    send_rows(last, distance(last))

    labcol[...] = jnp.full_like(labcol, -2)
    rowacc[...] = jnp.full_like(rowacc, -1.0)

    def take_labels(t):
        for h in range(2):
            row = lab_land[2 * t + h]
            column = jnp.transpose(jnp.broadcast_to(row, (half_tile, half_tile)))
            labcol[pl.ds(pl.multiple_of(t * tile + h * half_tile, half_tile), half_tile), :] = jnp.where(
                column < 0, -2, column)

    def take_rows(t):
        values = land[pl.ds(4 * t, 4)].reshape(tile, width).astype(jnp.float32)
        factor = lax.rsqrt(jnp.mean(values * values, axis=-1, keepdims=True) + 1e-06) / math.sqrt(width)
        units[pl.ds(pl.multiple_of(t * tile, tile), tile), :] = (values * factor).astype(jnp.bfloat16)

    def group(t, g, running, diagonal):
        rows = pl.ds(pl.multiple_of(g * span, span), span)
        old = units[rows, :]
        fresh = units[pl.ds(pl.multiple_of(t * tile, tile), tile), :]
        sim = lax.dot_general(
            old, fresh, (((1,), (1,)), ((), ())), preferred_element_type=jnp.float32)
        col = labcol[rows, :]
        acc = rowacc[rows, :]
        out = []
        for h in range(2):
            part = sim[:, h * half_tile:(h + 1) * half_tile]
            same = col == lab_land[2 * t + h]
            if diagonal:
                i = g * span + lax.broadcasted_iota(jnp.int32, part.shape, 0)
                j = t * tile + h * half_tile + lax.broadcasted_iota(jnp.int32, part.shape, 1)
                same = same & (i != j)
            part = jnp.where(same, part, -1.0)
            acc = jnp.maximum(acc, part)
            out.append(jnp.maximum(running[h], jnp.max(part, axis=0, keepdims=True)))
        return acc, tuple(out)

    def keep_group(t, g, running, diagonal):
        acc, running = group(t, g, running, diagonal)
        rowacc[pl.ds(pl.multiple_of(g * span, span), span), :] = acc
        return running

    floor = (jnp.full((1, half_tile), -1.0, jnp.float32),) * 2

    def labels_in(row):
        label_copy(chip, row).wait_recv()

    def rows_in(slot):
        block_copy(me, slot, slot).wait_recv()

    def take_tile(t, others, halves):
        for h in halves:
            labels_in(2 * t + h)
        take_labels(t)
        for s in others:
            rows_in(4 * t + s)
        take_rows(t)

    def whole_tile(t, others=(0, 1, 2, 3), halves=(0, 1)):
        take_tile(t, others, halves)
        running = lax.fori_loop(0, t // GROUP, lambda g, r: keep_group(t, g, r, False), floor)
        running = keep_group(t, t // GROUP, running, True)
        for h in range(2):
            colbest[2 * t + h] = running[h]

    def result_copy(row, dest, slot):
        return pltpu.make_async_remote_copy(
            src_ref=res_out.at[row],
            dst_ref=res_land.at[me],
            send_sem=res_send.at[slot],
            recv_sem=res_recv.at[me],
            device_id={OWNER: dest},
        )

    def give(t, k):
        for c in range(2):
            result_copy(2 * t, on_left(k) * 2 + c, t * 4 + c).start()
            result_copy(2 * t + 1, on_right(k) * 2 + c, t * 4 + 2 + c).start()

    def step(t, _):
        whole_tile(t)
        return 0

    lax.fori_loop(0, own, step, 0)
    keep.wait()
    whole_tile(own, (1 - core, 2, 3), (1,))
    lax.fori_loop(own + 1, last, step, 0)

    def left(slot, _):
        block_copy(me, slot, slot).wait_send()
        return 0

    def told(row, _):
        label_copy(chip, row).wait_send()
        return 0

    lax.fori_loop(0, 2 * own, told, 0)
    lax.fori_loop(2 * own + 1, chips, told, 0)

    lax.fori_loop(0, 4 * own + 1, left, 0)
    lax.fori_loop(4 * own + 2, 4 * last, left, 0)

    take_tile(last, (0, 1, 2, 3), (0, 1))
    square = (half_tile, half_tile)
    on_diagonal = lax.broadcasted_iota(jnp.int32, square, 0) == lax.broadcasted_iota(jnp.int32, square, 1)
    running = floor
    groups = far // GROUP
    for n in range(groups):
        g = (own // GROUP + n) % groups
        acc, running = group(last, g, running, g == last // GROUP)
        for m in range(2 * GROUP):
            i = 2 * GROUP * g + m
            best = jnp.max(acc[m * half_tile:(m + 1) * half_tile, :], axis=1, keepdims=True)
            row = jnp.max(jnp.where(on_diagonal, best, -1.0), axis=0, keepdims=True)
            if i // 2 == last:
                colbest[i] = row
            else:
                res_out[i] = jnp.maximum(colbest[i], row)
        if g == own // GROUP:
            for c in range(2):
                result_copy(2 * own + 1, opposite * 2 + c, 4 * own + 2 + c).start()
            result_copy(2 * own, partner, 4 * own).start()
            res_land[me] = res_out[2 * own]
        for t in range(GROUP * g, GROUP * (g + 1)):
            if t not in (own, last):
                give(t, distance(t))
    for h in range(2):
        res_out[2 * last + h] = jnp.maximum(colbest[2 * last + h], running[h])
    give(last, distance(last))

    def answered(slot, _):
        result_copy(0, me, slot).wait_send()
        return 0

    lax.fori_loop(4 * last, owners, left, 0)
    lax.fori_loop(0, 4 * own + 1, answered, 0)
    lax.fori_loop(4 * own + 2, owners, answered, 0)

    def back(i, _):
        s = lax.rem(me + i, owners)
        pltpu.make_async_remote_copy(
            src_ref=res_out.at[0], dst_ref=res_land.at[s], send_sem=res_send.at[0],
            recv_sem=res_recv.at[s], device_id={OWNER: s},
        ).wait_recv()
        return 0

    lax.fori_loop(1, owners, back, 0)

    for k in range(chips):
        low, high = res_land[2 * k], res_land[2 * k + 1]
        low = jnp.where(core == 0, low, pltpu.roll(low, cap, 1))
        high = jnp.where(core == 0, pltpu.roll(high, cap, 1), high)
        out_ref[k:k + 1, :] = jnp.where(lane < cap, low, high)


def on_device(embeddings, cluster, lengths):
    owners = lax.axis_size(OWNER)
    rows_here, width = embeddings.shape
    cap = rows_here // owners
    chips = owners // 2
    dma = pltpu.SemaphoreType.DMA
    out = pl.pallas_call(
        lambda *refs: exchange_kernel(owners, *refs),
        out_shape=jax.ShapeDtypeStruct((chips, 2 * cap), jnp.float32),
        in_specs=[
            pl.BlockSpec(memory_space=pltpu.SMEM),
            pl.BlockSpec(memory_space=pltpu.HBM),
            pl.BlockSpec(memory_space=pltpu.VMEM),
        ],
        out_specs=pl.BlockSpec(memory_space=pltpu.VMEM),
        scratch_shapes=[
            pltpu.VMEM((rows_here, width), jnp.bfloat16),
            pltpu.VMEM((2, 2 * cap, width), jnp.bfloat16),
            pltpu.VMEM((owners, cap, width), jnp.bfloat16),
            pltpu.VMEM((rows_here, width), jnp.bfloat16),
            pltpu.VMEM((2, chips, 1, cap), jnp.int32),
            pltpu.VMEM((chips, 1, cap), jnp.int32),
            pltpu.VMEM((chips, 1, 2 * cap), jnp.int32),
            pltpu.VMEM((chips, 1, 2 * cap), jnp.int32),
            pltpu.VMEM((rows_here, 2 * cap), jnp.int32),
            pltpu.VMEM((rows_here, 2 * cap), jnp.float32),
            pltpu.VMEM((chips, 1, 2 * cap), jnp.float32),
            pltpu.VMEM((chips, 1, 2 * cap), jnp.float32),
            pltpu.VMEM((owners, 1, 2 * cap), jnp.float32),
            dma((3,)), dma, dma((2,)),
            dma((owners,)), dma((owners,)), dma((chips,)), dma((chips,)), dma((owners,)), dma((owners,)),
            pltpu.SemaphoreType.REGULAR((chips // 2 - 1, 2)),
        ],
        compiler_params=pltpu.CompilerParams(
            collective_id=0, has_side_effects=True),
        cost_estimate=pl.CostEstimate(
            flops=2 * rows_here * rows_here * width, bytes_accessed=4 * rows_here * width, transcendentals=0),
    )(lengths, embeddings, cluster.reshape(chips, 2 * cap))
    return out.reshape(rows_here)


def solution(mesh):
    return jax.shard_map(
        on_device,
        mesh=mesh,
        in_specs=(P(("parts", OWNER), None), P(("parts", OWNER)), P(("parts", OWNER), None)),
        out_specs=P(("parts", OWNER)),
        check_vma=False,
    )
```
